128 devices in a mesh: row: 32 (over z, x, y_lo), col: 4 (over y_hi, core).
Axes of the slice: x: 4, y: 4 (y_hi: 2, y_lo: 2; y = y_hi * 2 + y_lo), z: 4, core: 2. Of those that a mesh axis runs over, the one named last changes fastest.
Arguments:
- trailing: float32 [65536, 8192], P('row', 'col'), may hold values from -6 to 6
- vectors: float32 [65536, 256], P(('row', 'col')), may hold values from -0.09375 to 0.09375
- tfactor: float32 [256, 256], replicated, may hold values from -0.375 to 0.375
Outputs:
- updated: float32 [65536, 8192], P('row', 'col')
The draws below stay inside these ranges and needn't reach their ends.
All inputs are finite; a program needn't handle non-finite values.
Results may differ from the reference program's by a relative error of at most 0.0003.
Values sent between devices are 32-bit elements.
A program may use at most 128 MiB of HBM per device.

```python
import jax
import jax.numpy as jnp
from jax import lax

N = 8192
K = 256
M = 65536


def steps_of(own_key, shape, shards, smallest, high):
    loudness, own = 1.0, jax.random.fold_in(own_key, 6)
    for axis_at, shards_of in shards:
        heights = jnp.exp(jax.random.uniform(jax.random.fold_in(own, axis_at), (shards_of,), jnp.float32, smallest / len(shards), high / len(shards)))
        loudness = loudness * jnp.repeat(heights, shape[axis_at] // shards_of).reshape([-1 if axis == axis_at else 1 for axis in range(len(shape))])
    return loudness


def gaussian(own_key, dims, width, most, split=(), kind=jnp.bfloat16):
    loudness = steps_of(own_key, dims, split, -0.22, 0.18) if split else 1.0
    drawn = jax.random.normal(own_key, dims, jnp.float32) * width * loudness
    return jnp.minimum(jnp.maximum(drawn, -most), most).astype(kind)


def setup_inputs(seed: int = 0) -> dict:
    arg_keys = jax.random.split(jax.random.key(seed), 4)
    return {
        "trailing": gaussian(arg_keys[0], (M, N), 1.0, 6.0, ((0, 32), (1, 4)), jnp.float32),
        "vectors": gaussian(arg_keys[1], (M, K), (M // 16) ** -0.5, 0.09375, ((0, 128),), jnp.float32),
        "tfactor": gaussian(arg_keys[2], (K, K), K ** -0.5, 0.375, (), jnp.float32),
    }


def reference(trailing, vectors, tfactor):
    high = lax.Precision.HIGHEST
    coeffs = jnp.dot(vectors.T, trailing, precision=high, preferred_element_type=jnp.float32)
    scaled = jnp.dot(tfactor, coeffs, precision=high, preferred_element_type=jnp.float32)
    return trailing - jnp.dot(vectors, scaled, precision=high, preferred_element_type=jnp.float32)
```

```python
import functools

import jax
import jax.numpy as jnp
from jax import lax
from jax.experimental import pallas as pl
from jax.experimental.pallas import tpu as pltpu
from jax.sharding import PartitionSpec as P

MESH = pl.DeviceIdType.MESH
F32, BF16 = jnp.float32, jnp.bfloat16
RING = 4
HALVES = 2
V_PIECES = 2
AWAY = (2, 1, 3)
OTHERS = ((0, 1), (1, 0), (3, 0), (1, 1), (3, 1), (2, 0), (2, 1))


def split(x):
    high = x.astype(BF16)
    return high, (x - high.astype(F32)).astype(BF16)


def dot(a, b):
    return jnp.dot(a, b, preferred_element_type=F32)


def dot3(a_high, a_low, b_high, b_low):
    return dot(a_high, b_high) + (dot(a_low, b_high) + dot(a_high, b_low))


def sum_kernel(
    c_hbm, v_hbm, t_hbm, c_ref, w_high, w_low, res,
    near, acc, vt, got1, got2, t_ref, c_sem, l_sem,
    sib_send, sib_recv, v_send, v_recv, f_send, f_recv,
    r1_send, r1_recv, r2_send, r2_recv, g2_send, g2_recv, g1_send, g1_recv,
):
    row, col = lax.axis_index("row"), lax.axis_index("col")
    core, y_hi = lax.rem(col, 2), lax.div(col, 2)
    z, x, y_lo = lax.div(row, 2 * RING), lax.rem(lax.div(row, 2), RING), lax.rem(row, 2)
    sibling = y_hi * 2 + (1 - core)
    across = (1 - y_hi) * 2 + core
    across_sibling = (1 - y_hi) * 2 + (1 - core)
    blocks, own, depth = near.shape
    chunks, height, width = c_ref.shape
    part = depth // HALVES
    sub = part // (2 * RING)
    pos, other = (x, z), (z, x)

    def wrap(i):
        return lax.rem(i + RING, RING)

    def target(d, away, across_other, flip):
        first = wrap(pos[d] + away)
        second = wrap(other[d] + across_other)
        zz, xx = (second, first) if d == 0 else (first, second)
        return (zz * (2 * RING) + xx * 2 + lax.rem(y_lo + flip, 2), col)

    def remote(src, dst, send, recv, to):
        return pltpu.make_async_remote_copy(
            src_ref=src, dst_ref=dst, send_sem=send, recv_sem=recv, device_id=to, device_id_type=MESH
        )

    def chunk_of(d, away):
        return d * RING + wrap(pos[d] + away)

    order = [(d, away) for away in AWAY + (0,) for d in range(2)]

    def c_copy(chunk):
        return pltpu.make_async_copy(
            c_hbm.at[:, pl.ds(pl.multiple_of(chunk * width, width), width)], c_ref.at[chunk], c_sem.at[chunk]
        )

    v_copy = pltpu.make_async_copy(v_hbm, near.at[col], l_sem.at[0])
    t_copy = pltpu.make_async_copy(t_hbm, t_ref, l_sem.at[1])
    v_copy.start()
    t_copy.start()
    for d, away in order:
        c_copy(chunk_of(d, away)).start()

    barrier = pltpu.get_barrier_semaphore()
    friends = [(row, sibling), (row, across)]
    friends += [target(d, away, 0, 0) for d in range(2) for away in AWAY]
    friends += [target(0, 0, q, 1) for q in range(RING)]
    friends += [target(1, 0, q, 1) for q in range(1, RING)]
    for friend in friends:
        pl.semaphore_signal(barrier, inc=1, device_id=friend, device_id_type=MESH)
    pl.semaphore_wait(barrier, len(friends))

    size = own // V_PIECES

    def v_copy_across(h, p):
        there = near.at[col, pl.ds(p * size, size), pl.ds(h * part, part)]
        return remote(there, there, v_send.at[h, p], v_recv.at[h, p], (row, across))

    def forward(h, p):
        there = near.at[across, pl.ds(p * size, size), pl.ds(h * part, part)]
        return remote(there, there, f_send.at[h, p], f_recv.at[h, p], (row, sibling))

    v_copy.wait()
    for h in range(HALVES):
        for p in range(V_PIECES):
            v_copy_across(h, p).start()
    sib = remote(near.at[col], near.at[col], sib_send, sib_recv, (row, sibling))
    sib.start()

    def keep(block, h):
        high, low = split(near[block, :, h * part:(h + 1) * part].T)
        vt[h, block, :part] = high
        vt[h, block, part:] = low

    def arrive(h):
        for p in range(V_PIECES):
            v_copy_across(h, p).wait()
            forward(h, p).start()
        keep(across, h)
        for p in range(V_PIECES):
            forward(h, p).wait()
        keep(across_sibling, h)

    def product(h, block, high, low):
        both = dot(vt[h, block], high)
        return both[:part] + (both[part:] + dot(vt[h, block, :part], low))

    def pieces_of(chunk, pair):
        return [(b, split(c_ref[chunk, pl.ds(pl.multiple_of(b * own, own), own)])) for b in pair]

    def near_job(chunk):
        (b0, c0), (b1, c1) = pieces_of(chunk, (col, sibling))
        for h in range(HALVES):
            acc[h, chunk] = product(h, b0, *c0) + product(h, b1, *c1)

    def job(chunk, h):
        (b0, c0), (b1, c1) = pieces_of(chunk, (across, across_sibling))
        acc[h, chunk] += product(h, b0, *c0) + product(h, b1, *c1)

    def weigh(block, t_high, t_low):
        high, low = split(near[block])
        rows = pl.ds(pl.multiple_of(block * own, own), own)
        w_high[rows], w_low[rows] = split(dot3(high, low, t_high, t_low))

    def r1_copy(h, d, i):
        chunk = chunk_of(d, AWAY[i])
        return remote(
            acc.at[h, chunk], got1.at[h, d, i], r1_send.at[h, d, i], r1_recv.at[h, d, i], target(d, AWAY[i], 0, 0)
        )

    def rows_of(d, e):
        q, flip = (0, 0) if e == 0 else OTHERS[e - 1]
        return wrap(other[d] - q) * 2 + lax.rem(y_lo + flip, 2)

    def r2_copy(h, d, e):
        q, flip = OTHERS[e - 1]
        place = wrap(other[d] + q) * 2 + lax.rem(y_lo + flip, 2)
        rows = pl.ds(pl.multiple_of(place * sub, sub), sub)
        return remote(
            acc.at[h, chunk_of(d, 0), rows], got2.at[h, d, e], r2_send.at[h, d, e], r2_recv.at[h, d, e],
            target(d, 0, q, flip),
        )

    def res_rows(h, d, e):
        return pl.ds(pl.multiple_of(h * part + rows_of(d, e) * sub, sub), sub)

    def g2_copy(h, d, e):
        q, flip = OTHERS[e - 1]
        ref = res.at[chunk_of(d, 0), res_rows(h, d, 0)]
        return remote(ref, ref, g2_send.at[h, d, e], g2_recv.at[h, d, e], target(d, 0, q, flip))

    def g1_copy(h, d, i, e):
        ref = res.at[chunk_of(d, 0), res_rows(h, d, e)]
        return remote(ref, ref, g1_send.at[h, d, i, e], g1_recv.at[h, d, i, e], target(d, AWAY[i], 0, 0))

    def produce(h):
        for d, away in order:
            job(chunk_of(d, away), h)
            if away:
                r1_copy(h, d, AWAY.index(away)).start()

    def collect(h):
        for d in range(2):
            mine = chunk_of(d, 0)
            for i in range(3):
                r1_copy(h, d, i).wait_recv()
            acc[h, mine] += got1[h, d, 0] + (got1[h, d, 1] + got1[h, d, 2])
            for e in range(1, 2 * RING):
                r2_copy(h, d, e).start()

    def finish(h):
        for d in range(2):
            mine = chunk_of(d, 0)
            for e in range(1, 2 * RING):
                r2_copy(h, d, e).wait_recv()
            total = acc[h, mine, pl.ds(pl.multiple_of(rows_of(d, 0) * sub, sub), sub)]
            for e in range(1, 2 * RING):
                total += got2[h, d, e]
            res[mine, res_rows(h, d, 0)] = total
            for e in range(1, 2 * RING):
                g2_copy(h, d, e).start()
            for i in range(3):
                g1_copy(h, d, i, 0).start()

    def spread(h):
        for e in range(1, 2 * RING):
            for d in range(2):
                g2_copy(h, d, e).wait_recv()
                for i in range(3):
                    g1_copy(h, d, i, e).start()

    def gathered(h):
        for e in range(2 * RING):
            for d in range(2):
                for i in range(3):
                    g1_copy(h, d, i, e).wait_recv()

    for h in range(HALVES):
        keep(col, h)
    t_copy.wait()
    sib.wait()
    for h in range(HALVES):
        keep(sibling, h)
    for d, away in order:
        chunk = chunk_of(d, away)
        c_copy(chunk).wait()
        near_job(chunk)
    t_high, t_low = split(t_ref[...])
    weigh(col, t_high, t_low)
    arrive(0)
    produce(0)
    weigh(sibling, t_high, t_low)
    arrive(1)
    produce(1)
    collect(0)
    weigh(across, t_high, t_low)
    finish(0)
    weigh(across_sibling, t_high, t_low)
    collect(1)
    spread(0)
    finish(1)
    spread(1)
    gathered(0)
    gathered(1)

    for h in range(HALVES):
        for d in range(2):
            for i in range(3):
                r1_copy(h, d, i).wait_send()
                for e in range(2 * RING):
                    g1_copy(h, d, i, e).wait_send()
            for e in range(1, 2 * RING):
                r2_copy(h, d, e).wait_send()
                g2_copy(h, d, e).wait_send()


def update_kernel(c_ref, w_high, w_low, res, out_hbm, stage, sem):
    chunks, height, width = c_ref.shape
    slots = stage.shape[0]
    own = height // 4

    def out_copy(chunk, slot):
        return pltpu.make_async_copy(
            stage.at[slot], out_hbm.at[:, pl.ds(pl.multiple_of(chunk * width, width), width)], sem.at[slot]
        )

    def step(chunk, carry):
        slot = lax.rem(chunk, slots)

        @pl.when(chunk >= slots)
        def _():
            out_copy(chunk - slots, slot).wait()

        high, low = split(res[chunk])
        for b in range(4):
            rows = pl.ds(b * own, own)
            stage[slot, rows] = c_ref[chunk, rows] - dot3(w_high[rows], w_low[rows], high, low)
        out_copy(chunk, slot).start()
        return carry

    lax.fori_loop(0, chunks, step, 0)
    for i in range(slots):
        chunk = chunks - slots + i
        out_copy(chunk, chunk % slots).wait()


def grid_shards(trailing, vectors, tfactor):
    height, columns = trailing.shape
    own, depth = vectors.shape
    chunks = 2 * RING
    width = columns // chunks
    blocks = height // own
    part = depth // HALVES
    sub = part // (2 * RING)
    dma = pltpu.SemaphoreType.DMA
    vmem = pl.BlockSpec(memory_space=pltpu.VMEM)
    hbm = pl.BlockSpec(memory_space=pl.ANY)
    held, w_high, w_low, res = pl.pallas_call(
        sum_kernel,
        out_shape=(
            pltpu.VMEM((chunks, height, width), F32),
            pltpu.VMEM((height, depth), BF16),
            pltpu.VMEM((height, depth), BF16),
            pltpu.VMEM((chunks, depth, width), F32),
        ),
        in_specs=[hbm, hbm, hbm],
        out_specs=(vmem, vmem, vmem, vmem),
        scratch_shapes=[
            pltpu.VMEM((blocks, own, depth), F32),
            pltpu.VMEM((HALVES, chunks, part, width), F32),
            pltpu.VMEM((HALVES, blocks, 2 * part, own), BF16),
            pltpu.VMEM((HALVES, 2, 3, part, width), F32),
            pltpu.VMEM((HALVES, 2, 2 * RING, sub, width), F32),
            pltpu.VMEM((depth, depth), F32),
            dma((chunks,)), dma((2,)),
            dma, dma,
            dma((HALVES, V_PIECES)), dma((HALVES, V_PIECES)), dma((HALVES, V_PIECES)), dma((HALVES, V_PIECES)),
            dma((HALVES, 2, 3)), dma((HALVES, 2, 3)),
            dma((HALVES, 2, 2 * RING)), dma((HALVES, 2, 2 * RING)),
            dma((HALVES, 2, 2 * RING)), dma((HALVES, 2, 2 * RING)),
            dma((HALVES, 2, 3, 2 * RING)), dma((HALVES, 2, 3, 2 * RING)),
        ],
        compiler_params=pltpu.CompilerParams(
            collective_id=0, has_side_effects=True, vmem_limit_bytes=20 << 20
        ),
    )(trailing, vectors, tfactor)
    slots = 4
    return pl.pallas_call(
        update_kernel,
        out_shape=jax.ShapeDtypeStruct((height, columns), F32),
        in_specs=[vmem, vmem, vmem, vmem],
        out_specs=hbm,
        scratch_shapes=[pltpu.VMEM((slots, height, width), F32), dma((slots,))],
        compiler_params=pltpu.CompilerParams(vmem_limit_bytes=20 << 20),
    )(held, w_high, w_low, res)


def plain_shards(trailing, vectors, tfactor):
    dot = functools.partial(jnp.dot, precision=lax.Precision.HIGH, preferred_element_type=F32)
    near_vectors = lax.all_gather(vectors, "col", axis=0, tiled=True)
    summed = lax.psum(dot(near_vectors.T, trailing), "row")
    return trailing - dot(near_vectors, dot(tfactor, summed))


def solution(mesh):
    placed = (P("row", "col"), P(("row", "col"), None), P())
    fits = mesh.shape["row"] == 2 * RING * RING and mesh.shape["col"] == 4

    def shards(trailing, vectors, tfactor):
        if fits and trailing.shape == (2048, 2048) and vectors.shape == (512, 256):
            return grid_shards(trailing, vectors, tfactor)
        return plain_shards(trailing, vectors, tfactor)

    return jax.shard_map(
        shards, mesh=mesh, in_specs=placed, out_specs=P("row", "col"), check_vma=False
    )
```

```python
import functools

import jax
import jax.numpy as jnp
from jax import lax
from jax.experimental import pallas as pl
from jax.experimental.pallas import tpu as pltpu
from jax.sharding import PartitionSpec as P

MESH = pl.DeviceIdType.MESH
F32, BF16 = jnp.float32, jnp.bfloat16
RING = 4
HALVES = 2
V_PIECES = 2
WAYS = (1, -1)
OTHERS = (0, 1, -1, 2)


def split(x):
    high = x.astype(BF16)
    return high, (x - high.astype(F32)).astype(BF16)


def dot(a, b):
    return jnp.dot(a, b, preferred_element_type=F32)


def dot3(a_high, a_low, b_high, b_low):
    return dot(a_high, b_high) + (dot(a_low, b_high) + dot(a_high, b_low))


def stacked(x):
    high, low = split(x)
    return jnp.concatenate([high, high, low], axis=0)


def sum_kernel(
    c_hbm, v_hbm, t_hbm, c_ref, w_ref, res,
    near, acc, vt, passing, got1, got2, got3, t_ref, c_sem, l_sem,
    send, sib_recv, v_recv, f_recv, a_recv, r1_recv, r2_recv, y_recv, g2_recv, g1_recv, near_recv, far_recv,
):
    row, col = lax.axis_index("row"), lax.axis_index("col")
    core, y_hi = lax.rem(col, 2), lax.div(col, 2)
    z, x, y_lo = lax.div(row, 2 * RING), lax.rem(lax.div(row, 2), RING), lax.rem(row, 2)
    sibling = y_hi * 2 + (1 - core)
    across = (1 - y_hi) * 2 + core
    across_sibling = (1 - y_hi) * 2 + (1 - core)
    blocks, own, depth = near.shape
    chunks, height, width = c_ref.shape
    part = depth // HALVES
    sub = part // RING
    half = part // 2
    group = range(1, RING)
    dims = range(2)
    pos, other = (x, z), (z, x)

    def wrap(i):
        return lax.rem(i + RING, RING)

    def target(d, away, across_other, flip):
        first = wrap(pos[d] + away)
        second = wrap(other[d] + across_other)
        zz, xx = (second, first) if d == 0 else (first, second)
        return (zz * (2 * RING) + xx * 2 + lax.rem(y_lo + flip, 2), col)

    def remote(src, dst, recv, to):
        return pltpu.make_async_remote_copy(
            src_ref=src, dst_ref=dst, send_sem=send, recv_sem=recv, device_id=to, device_id_type=MESH
        )

    def take(ref, sem):
        pltpu.make_async_copy(ref, ref, sem).wait()

    def chunk_of(d, away):
        return d * RING + wrap(pos[d] + away)

    order = [(d, away) for away in (2, 1, -1, 0) for d in dims]

    def c_copy(i):
        chunk = chunk_of(*order[i])
        return pltpu.make_async_copy(
            c_hbm.at[:, pl.ds(pl.multiple_of(chunk * width, width), width)], c_ref.at[chunk], c_sem.at[i]
        )

    v_copy = pltpu.make_async_copy(v_hbm, near.at[col], l_sem.at[0])
    t_copy = pltpu.make_async_copy(t_hbm, t_ref, l_sem.at[1])
    v_copy.start()
    t_copy.start()

    barrier = pltpu.get_barrier_semaphore()
    friends = [(row, sibling), (row, across)]
    friends += [target(d, away, 0, 0) for d in dims for away in (1, -1, 2)]
    friends += [target(0, 0, 0, 1)]
    for friend in friends:
        pl.semaphore_signal(barrier, inc=1, device_id=friend, device_id_type=MESH)
    v_copy.wait()
    t_copy.wait()
    for i in range(chunks):
        c_copy(i).start()
    pl.semaphore_wait(barrier, len(friends))

    size = own // V_PIECES

    def v_copy_across(h, p):
        there = near.at[col, pl.ds(p * size, size), pl.ds(h * part, part)]
        return remote(there, there, v_recv.at[h, p], (row, across))

    def forward(h, p):
        there = near.at[across, pl.ds(p * size, size), pl.ds(h * part, part)]
        return remote(there, there, f_recv.at[h], (row, sibling))

    for h in range(HALVES):
        for p in range(V_PIECES):
            v_copy_across(h, p).start()
    sib = remote(near.at[col], near.at[col], sib_recv, (row, sibling))
    sib.start()

    def keep(block, h):
        high, low = split(near[block, :, h * part:(h + 1) * part].T)
        vt[h, block, :part] = high
        vt[h, block, part:] = low

    def arrive(h):
        for p in range(V_PIECES):
            v_copy_across(h, p).wait_recv()
            forward(h, p).start()
        keep(across, h)

    def arrive_sibling(h):
        take(near.at[across_sibling, :, pl.ds(h * part, part)], f_recv.at[h])
        keep(across_sibling, h)

    def product(h, block, high, low):
        both = dot(vt[h, block], high)
        return both[:part] + (both[part:] + dot(vt[h, block, :part], low))

    def pieces_of(chunk, pair):
        return [(b, split(c_ref[chunk, pl.ds(pl.multiple_of(b * own, own), own)])) for b in pair]

    def near_job(chunk):
        (b0, c0), (b1, c1) = pieces_of(chunk, (col, sibling))
        for h in range(HALVES):
            acc[h, chunk] = product(h, b0, *c0) + product(h, b1, *c1)

    def job(chunk, h):
        (b0, c0), (b1, c1) = pieces_of(chunk, (across, across_sibling))
        acc[h, chunk] += product(h, b0, *c0) + product(h, b1, *c1)

    def weigh(block):
        t_high, t_low = split(t_ref[...])
        high, low = split(near[block])
        high, low = split(dot3(high, low, t_high, t_low))
        rows = pl.ds(pl.multiple_of(block * own, own), own)
        for h in range(HALVES):
            lanes = slice(h * part, (h + 1) * part)
            first = 3 * h * part
            w_ref[rows, first:first + part] = high[:, lanes]
            w_ref[rows, first + part:first + 2 * part] = low[:, lanes]
            w_ref[rows, first + 2 * part:first + 3 * part] = high[:, lanes]

    def upper(way):
        return slice(0, half) if way == 0 else slice(half, part)

    def lower(way):
        return slice(half, part) if way == 0 else slice(0, half)

    def a_copy(h, d, way):
        return remote(
            acc.at[h, chunk_of(d, 2), upper(way)], passing.at[h, d, way],
            a_recv.at[h, d, way], target(d, WAYS[way], 0, 0),
        )

    def b_copy(h, d, way):
        return remote(
            acc.at[h, chunk_of(d, WAYS[way]), lower(way)], got1.at[h, d, way, lower(way)],
            r1_recv.at[h, d], target(d, WAYS[way], 0, 0),
        )

    def s_copy(h, d, way):
        return remote(
            acc.at[h, chunk_of(d, WAYS[way]), upper(way)], got1.at[h, d, way, upper(way)],
            r1_recv.at[h, d], target(d, WAYS[way], 0, 0),
        )

    def place_rows(d, away):
        return pl.ds(pl.multiple_of(wrap(other[d] + away) * sub, sub), sub)

    def r2_copy(h, d, e):
        return remote(
            acc.at[h, chunk_of(d, 0), place_rows(d, OTHERS[e])], got2.at[h, d, e - 1], r2_recv.at[h, d],
            target(d, 0, OTHERS[e], 0),
        )

    def y_copy(h, d):
        return remote(
            acc.at[h, chunk_of(d, 0), place_rows(d, 0)], got3.at[h, d], y_recv.at[h, d], target(d, 0, 0, 1)
        )

    def res_rows(h, d, e):
        return pl.ds(pl.multiple_of(h * part + wrap(other[d] - OTHERS[e]) * sub, sub), sub)

    def g2_copy(h, d, e):
        ref = res.at[chunk_of(d, 0), res_rows(h, d, 0)]
        return remote(ref, ref, g2_recv.at[h, d, e], target(d, 0, OTHERS[e], 0))

    def g1_copy(h, d, way, e):
        ref = res.at[chunk_of(d, 0), res_rows(h, d, e)]
        recv = g1_recv.at[h, d, e] if way == e % 2 else near_recv.at[h]
        return remote(ref, ref, recv, target(d, WAYS[way], 0, 0))

    def gf_copy(h, d, e):
        way = e % 2
        ref = res.at[chunk_of(d, -WAYS[way]), res_rows(h, d, e)]
        return remote(ref, ref, far_recv.at[h], target(d, WAYS[way], 0, 0))

    def produce(h):
        for d in dims:
            job(chunk_of(d, 2), h)
        for d in dims:
            for way in range(2):
                a_copy(h, d, way).start()
        for way in range(2):
            for d in dims:
                job(chunk_of(d, WAYS[way]), h)
            for d in dims:
                b_copy(h, d, way).start()
        for d in dims:
            job(chunk_of(d, 0), h)

    def pass_on(h):
        for d in dims:
            for way in range(2):
                a_copy(h, d, way).wait_recv()
                acc[h, chunk_of(d, WAYS[way]), upper(way)] += passing[h, d, way]
                s_copy(h, d, way).start()

    def collect(h):
        for d in dims:
            mine = chunk_of(d, 0)
            take(got1.at[h, d], r1_recv.at[h, d])
            acc[h, mine] += got1[h, d, 0] + got1[h, d, 1]
            for e in group:
                r2_copy(h, d, e).start()

    def pair(h):
        for d in dims:
            take(got2.at[h, d], r2_recv.at[h, d])
            acc[h, chunk_of(d, 0), place_rows(d, 0)] += got2[h, d, 0] + (got2[h, d, 1] + got2[h, d, 2])
            y_copy(h, d).start()

    def finish(h):
        for d in dims:
            mine = chunk_of(d, 0)
            y_copy(h, d).wait_recv()
            res[mine, res_rows(h, d, 0)] = acc[h, mine, place_rows(d, 0)] + got3[h, d]
            for e in group:
                g2_copy(h, d, e).start()
            for way in range(2):
                g1_copy(h, d, way, 0).start()

    def spread(h, e):
        for d in dims:
            g2_copy(h, d, e).wait_recv()
            for way in range(2):
                g1_copy(h, d, way, e).start()

    def hand_on(h, e):
        for d in dims:
            g1_copy(h, d, e % 2, e).wait_recv()
            gf_copy(h, d, e).start()

    def near_gathered(h):
        take(res.at[0], near_recv.at[h])

    def far_gathered(h):
        take(res.at[0], far_recv.at[h])

    def update(chunk):
        right = stacked(res[chunk, :part])
        for b in range(blocks):
            rows = slice(b * own, (b + 1) * own)
            c_ref[chunk, rows] = c_ref[chunk, rows] - dot(w_ref[rows, :3 * part], right)

    for h in range(HALVES):
        keep(col, h)
    weigh(col)
    take(near.at[sibling], sib_recv)
    for h in range(HALVES):
        keep(sibling, h)
    for i in range(chunks):
        c_copy(i).wait()
        near_job(chunk_of(*order[i]))
    arrive(0)
    arrive_sibling(0)
    produce(0)
    weigh(sibling)
    arrive(1)
    pass_on(0)
    arrive_sibling(1)
    produce(1)
    collect(0)
    pass_on(1)
    weigh(across)
    weigh(across_sibling)
    pair(0)
    collect(1)
    finish(0)
    pair(1)
    for e in group:
        spread(0, e)
    finish(1)
    for d in dims:
        update(chunk_of(d, 0))
    for e in range(RING):
        hand_on(0, e)
    for e in group:
        spread(1, e)
    near_gathered(0)
    hand_on(1, 0)
    for d in dims:
        update(chunk_of(d, 1))
    hand_on(1, 1)
    hand_on(1, 2)
    for d in dims:
        update(chunk_of(d, -1))
    hand_on(1, 3)
    far_gathered(0)
    for d in dims:
        update(chunk_of(d, 2))
    near_gathered(1)
    far_gathered(1)

    take(near.at[pl.ds(0, 3)], send)
    for h in range(HALVES):
        take(passing.at[h], send)
        take(got1.at[h], send)
        take(got2.at[h], send)
        take(got3.at[h], send)
        take(got2.at[h], send)
        take(res.at[pl.ds(0, 3)], send)


def update_kernel(c_ref, w_ref, res, out_hbm, stage, sem):
    chunks, height, width = c_ref.shape
    part = res.shape[1] // HALVES
    slots = stage.shape[0]
    pieces = 4
    size = height // pieces

    def out_copy(chunk, slot):
        return pltpu.make_async_copy(
            stage.at[slot], out_hbm.at[:, pl.ds(pl.multiple_of(chunk * width, width), width)], sem.at[slot]
        )

    def step(chunk, carry):
        slot = lax.rem(chunk, slots)

        @pl.when(chunk >= slots)
        def _():
            out_copy(chunk - slots, slot).wait()

        right = stacked(res[chunk, part:])
        for p in range(pieces):
            rows = slice(p * size, (p + 1) * size)
            stage[slot, rows] = c_ref[chunk, rows] - dot(w_ref[rows, 3 * part:], right)
        out_copy(chunk, slot).start()
        return carry

    lax.fori_loop(0, chunks, step, 0)
    for i in range(slots):
        chunk = chunks - slots + i
        out_copy(chunk, chunk % slots).wait()


def grid_shards(trailing, vectors, tfactor):
    height, columns = trailing.shape
    own, depth = vectors.shape
    chunks = 2 * RING
    width = columns // chunks
    blocks = height // own
    part = depth // HALVES
    sub = part // RING
    dma = pltpu.SemaphoreType.DMA
    vmem = pl.BlockSpec(memory_space=pltpu.VMEM)
    hbm = pl.BlockSpec(memory_space=pltpu.HBM)
    held, w_ref, res = pl.pallas_call(
        sum_kernel,
        out_shape=(
            pltpu.VMEM((chunks, height, width), F32),
            pltpu.VMEM((height, 3 * depth), BF16),
            pltpu.VMEM((chunks, depth, width), F32),
        ),
        in_specs=[hbm, hbm, hbm],
        out_specs=(vmem, vmem, vmem),
        scratch_shapes=[
            pltpu.VMEM((blocks, own, depth), F32),
            pltpu.VMEM((HALVES, chunks, part, width), F32),
            pltpu.VMEM((HALVES, blocks, 2 * part, own), BF16),
            pltpu.VMEM((HALVES, 2, 2, part // 2, width), F32),
            pltpu.VMEM((HALVES, 2, 2, part, width), F32),
            pltpu.VMEM((HALVES, 2, RING - 1, sub, width), F32),
            pltpu.VMEM((HALVES, 2, sub, width), F32),
            pltpu.VMEM((depth, depth), F32),
            dma((chunks,)), dma((2,)),
            dma, dma, dma((HALVES, V_PIECES)), dma((HALVES,)),
            dma((HALVES, 2, 2)), dma((HALVES, 2)), dma((HALVES, 2)), dma((HALVES, 2)),
            dma((HALVES, 2, RING)), dma((HALVES, 2, RING)), dma((HALVES,)), dma((HALVES,)),
        ],
        compiler_params=pltpu.CompilerParams(
            collective_id=0, has_side_effects=True, vmem_limit_bytes=42 << 20
        ),
    )(trailing, vectors, tfactor)
    slots = 4
    return pl.pallas_call(
        update_kernel,
        out_shape=jax.ShapeDtypeStruct((height, columns), F32),
        in_specs=[vmem, vmem, vmem],
        out_specs=hbm,
        scratch_shapes=[pltpu.VMEM((slots, height, width), F32), dma((slots,))],
        compiler_params=pltpu.CompilerParams(vmem_limit_bytes=20 << 20),
    )(held, w_ref, res)


def plain_shards(trailing, vectors, tfactor):
    dot = functools.partial(jnp.dot, precision=lax.Precision.HIGH, preferred_element_type=F32)
    near_vectors = lax.all_gather(vectors, "col", axis=0, tiled=True)
    summed = lax.psum(dot(near_vectors.T, trailing), "row")
    return trailing - dot(near_vectors, dot(tfactor, summed))


def solution(mesh):
    placed = (P("row", "col"), P(("row", "col"), None), P())
    fits = mesh.shape["row"] == 2 * RING * RING and mesh.shape["col"] == 4

    def shards(trailing, vectors, tfactor):
        if fits and trailing.shape == (2048, 2048) and vectors.shape == (512, 256):
            return grid_shards(trailing, vectors, tfactor)
        return plain_shards(trailing, vectors, tfactor)

    return jax.shard_map(
        shards, mesh=mesh, in_specs=placed, out_specs=P("row", "col"), check_vma=False
    )
```

```python
import functools

import jax
import jax.numpy as jnp
from jax import lax
from jax.experimental import pallas as pl
from jax.experimental.pallas import tpu as pltpu
from jax.sharding import PartitionSpec as P

MESH = pl.DeviceIdType.MESH
F32, BF16 = jnp.float32, jnp.bfloat16
RING = 4
HALF = 128
PARTS = ((0, 128), (128, 64), (192, 64))
DIRECT = (False, False, True)
V_PIECES = 2
WAYS = (1, -1)
OTHERS = (0, 1, -1, 2)


def split(x):
    high = x.astype(BF16)
    return high, (x - high.astype(F32)).astype(BF16)


def dot(a, b):
    return jnp.dot(a, b, preferred_element_type=F32)


def dot3(a_high, a_low, b_high, b_low):
    return dot(a_high, b_high) + (dot(a_low, b_high) + dot(a_high, b_low))


def stacked_halves(ref, chunk, first, count):
    rows = []
    for at in range(first, first + count, HALF):
        high, low = split(ref[chunk, at:at + HALF])
        rows += [high, high, low]
    return jnp.concatenate(rows, axis=0)


def sum_kernel(
    c_hbm, v_hbm, t_hbm, c_ref, w_ref, res,
    v_ref, near, acc, vt, vt_far, c_high, c_low, passing, got1, far1, got2, got3, t_ref, c_sem, l_sem,
    send, sib_recv, v_recv, f_recv, a_recv, r1_recv, r2_recv, y_recv, g2_recv, g1_recv, near_recv, far_recv,
):
    row, col = lax.axis_index("row"), lax.axis_index("col")
    core, y_hi = lax.rem(col, 2), lax.div(col, 2)
    z, x, y_lo = lax.div(row, 2 * RING), lax.rem(lax.div(row, 2), RING), lax.rem(row, 2)
    sibling = y_hi * 2 + (1 - core)
    across = (1 - y_hi) * 2 + core
    across_sibling = (1 - y_hi) * 2 + (1 - core)
    blocks, depth, own = near.shape
    chunks, height, width = c_ref.shape
    group = range(1, RING)
    dims = range(2)
    pos, other = (x, z), (z, x)

    def wrap(i):
        return lax.rem(i + RING, RING)

    def target(d, away, across_other, flip):
        first = wrap(pos[d] + away)
        second = wrap(other[d] + across_other)
        zz, xx = (second, first) if d == 0 else (first, second)
        return (zz * (2 * RING) + xx * 2 + lax.rem(y_lo + flip, 2), col)

    def remote(src, dst, recv, to):
        return pltpu.make_async_remote_copy(
            src_ref=src, dst_ref=dst, send_sem=send, recv_sem=recv, device_id=to, device_id_type=MESH
        )

    def take(ref, sem):
        pltpu.make_async_copy(ref, ref, sem).wait()

    def chunk_of(d, away):
        return d * RING + wrap(pos[d] + away)

    order = [(d, away) for away in (2, 1, -1, 0) for d in dims]

    def c_copy(i):
        chunk = chunk_of(*order[i])
        return pltpu.make_async_copy(
            c_hbm.at[:, pl.ds(pl.multiple_of(chunk * width, width), width)], c_ref.at[chunk], c_sem.at[i]
        )

    v_copy = pltpu.make_async_copy(v_hbm, v_ref, l_sem.at[0])
    t_copy = pltpu.make_async_copy(t_hbm, t_ref, l_sem.at[1])
    v_copy.start()
    t_copy.start()

    barrier = pltpu.get_barrier_semaphore()
    friends = [(row, sibling), (row, across)]
    friends += [target(d, away, 0, 0) for d in dims for away in (1, -1, 2)]
    friends += [target(0, 0, 0, 1)]
    for friend in friends:
        pl.semaphore_signal(barrier, inc=1, device_id=friend, device_id_type=MESH)
    v_copy.wait()
    t_copy.wait()
    for i in range(chunks):
        c_copy(i).start()
    pl.semaphore_wait(barrier, len(friends))

    def rows_in(h, share=1, place=0):
        first, count = PARTS[h]
        return pl.ds(pl.multiple_of(first // share + place * (count // share), 8), count // share)

    def v_copy_across(h, p):
        size = own // V_PIECES
        there = near.at[col, rows_in(h), pl.ds(p * size, size)]
        return remote(there, there, v_recv.at[h, p], (row, across))

    def forward(h, p):
        size = own // V_PIECES
        there = near.at[across, rows_in(h), pl.ds(p * size, size)]
        return remote(there, there, f_recv.at[h], (row, sibling))

    for h, (first, count) in enumerate(PARTS):
        for at in range(-(-first // HALF) * HALF, first + count, HALF):
            near[col, at:at + HALF] = v_ref[:, at:at + HALF].T
        for p in range(V_PIECES):
            v_copy_across(h, p).start()
    sib = remote(near.at[col], near.at[col], sib_recv, (row, sibling))
    sib.start()

    def keep(ref, block, first, count, lanes=slice(None)):
        high, low = split(near[block, first:first + count])
        ref[2 * first:2 * first + count, lanes] = high
        ref[2 * first + count:2 * (first + count), lanes] = low

    def arrive(h):
        for p in range(V_PIECES):
            v_copy_across(h, p).wait_recv()
            forward(h, p).start()
        keep(vt_far, across, *PARTS[h], slice(0, own))

    def arrive_sibling(h):
        take(near.at[across_sibling, rows_in(h)], f_recv.at[h])
        keep(vt_far, across_sibling, *PARTS[h], slice(own, 2 * own))

    def product(ref, first, count, high, low):
        both = dot(ref[2 * first:2 * (first + count)], high)
        return both[:count] + (both[count:] + dot(ref[2 * first:2 * first + count], low))

    def piece(away, block):
        rows = pl.ds(pl.multiple_of(block * own, own), own)
        return split(jnp.concatenate([c_ref[chunk_of(d, away), rows] for d in dims], axis=1))

    def near_job(away):
        c0, c1 = piece(away, col), piece(away, sibling)
        for first in range(0, depth, HALF):
            total = product(vt.at[0], first, HALF, *c0) + product(vt.at[1], first, HALF, *c1)
            for d in dims:
                acc[chunk_of(d, away), first:first + HALF] = total[:, d * width:(d + 1) * width]

    def prepare(away):
        for i, block in enumerate((across, across_sibling)):
            c_high[away, i * own:(i + 1) * own], c_low[away, i * own:(i + 1) * own] = piece(away, block)

    def job(away, h, which=slice(None)):
        first, count = PARTS[h]
        total = product(vt_far.at[:, which], first, count, c_high[away, which], c_low[away, which])
        for d in dims:
            acc[chunk_of(d, away), first:first + count] += total[:, d * width:(d + 1) * width]

    def weigh(block):
        t_high, t_low = split(t_ref[...].T)
        high, low = split(near[block])
        high, low = split(dot3(t_high, t_low, high, low).T)
        rows = pl.ds(pl.multiple_of(block * own, own), own)
        for first in range(0, depth, HALF):
            lanes = slice(first, first + HALF)
            w_ref[rows, 3 * first:3 * first + HALF] = high[:, lanes]
            w_ref[rows, 3 * first + HALF:3 * first + 2 * HALF] = low[:, lanes]
            w_ref[rows, 3 * first + 2 * HALF:3 * (first + HALF)] = high[:, lanes]

    def half_rows(h, way):
        first, count = PARTS[h]
        return pl.ds(first + way * (count // 2), count // 2)

    def upper(h, way):
        return half_rows(h, way)

    def lower(h, way):
        return half_rows(h, 1 - way)

    def a_copy(h, d, way):
        return remote(
            acc.at[chunk_of(d, 2), upper(h, way)], passing.at[d, way, rows_in(h, 2)],
            a_recv.at[h, d, way], target(d, WAYS[way], 0, 0),
        )

    def b_copy(h, d, way):
        rows = rows_in(h) if DIRECT[h] else lower(h, way)
        return remote(
            acc.at[chunk_of(d, WAYS[way]), rows], got1.at[d, way, rows], r1_recv.at[h, d], target(d, WAYS[way], 0, 0)
        )

    def s_copy(h, d, way):
        rows = upper(h, way)
        return remote(
            acc.at[chunk_of(d, WAYS[way]), rows], got1.at[d, way, rows], r1_recv.at[h, d], target(d, WAYS[way], 0, 0)
        )

    def far_copy(h, d):
        return remote(
            acc.at[chunk_of(d, 2), rows_in(h)], far1.at[d, rows_in(h)], a_recv.at[h, d, 0], target(d, 2, 0, 0)
        )

    def place_rows(h, d, away):
        first, count = PARTS[h]
        sub = count // RING
        return pl.ds(pl.multiple_of(first + wrap(other[d] + away) * sub, sub), sub)

    def r2_copy(h, d, e):
        return remote(
            acc.at[chunk_of(d, 0), place_rows(h, d, OTHERS[e])], got2.at[d, e - 1, rows_in(h, RING)], r2_recv.at[h, d],
            target(d, 0, OTHERS[e], 0),
        )

    def y_copy(h, d):
        return remote(
            acc.at[chunk_of(d, 0), place_rows(h, d, 0)], got3.at[d, rows_in(h, RING)], y_recv.at[h, d],
            target(d, 0, 0, 1),
        )

    def g2_copy(h, d, e):
        ref = res.at[chunk_of(d, 0), place_rows(h, d, 0)]
        return remote(ref, ref, g2_recv.at[h, d, e], target(d, 0, OTHERS[e], 0))

    def g1_copy(h, d, way, e):
        ref = res.at[chunk_of(d, 0), place_rows(h, d, -OTHERS[e])]
        recv = g1_recv.at[h, d, e] if way == e % 2 and not DIRECT[h] else near_recv.at[h]
        return remote(ref, ref, recv, target(d, WAYS[way], 0, 0))

    def gf_copy(h, d, e):
        way = e % 2
        chunk = chunk_of(d, 0) if DIRECT[h] else chunk_of(d, -WAYS[way])
        ref = res.at[chunk, place_rows(h, d, -OTHERS[e])]
        return remote(ref, ref, far_recv.at[h], target(d, 2 if DIRECT[h] else WAYS[way], 0, 0))

    def produce(h):
        job(2, h, slice(0, own))
        arrive_sibling(h)
        job(2, h, slice(own, 2 * own))
        for d in dims:
            if DIRECT[h]:
                far_copy(h, d).start()
            else:
                for way in range(2):
                    a_copy(h, d, way).start()
        for way in range(2):
            job(WAYS[way] % RING, h)
            for d in dims:
                b_copy(h, d, way).start()
        job(0, h)

    def pass_on(h):
        for d in dims:
            for way in range(2):
                a_copy(h, d, way).wait_recv()
                acc[chunk_of(d, WAYS[way]), upper(h, way)] += passing[d, way, rows_in(h, 2)]
                s_copy(h, d, way).start()

    def collect(h):
        rows = rows_in(h)
        for d in dims:
            take(got1.at[d, :, rows], r1_recv.at[h, d])
            total = got1[d, 0, rows] + got1[d, 1, rows]
            if DIRECT[h]:
                take(far1.at[d, rows], a_recv.at[h, d, 0])
                total += far1[d, rows]
            acc[chunk_of(d, 0), rows] += total
            for e in group:
                r2_copy(h, d, e).start()

    def pair(h):
        rows = rows_in(h, RING)
        for d in dims:
            take(got2.at[d, :, rows], r2_recv.at[h, d])
            acc[chunk_of(d, 0), place_rows(h, d, 0)] += got2[d, 0, rows] + (got2[d, 1, rows] + got2[d, 2, rows])
            y_copy(h, d).start()

    def send_on(h, d, e):
        if DIRECT[h]:
            gf_copy(h, d, e).start()
        for way in range(2):
            g1_copy(h, d, way, e).start()

    def finish(h):
        for d in dims:
            mine = chunk_of(d, 0)
            y_copy(h, d).wait_recv()
            res[mine, place_rows(h, d, 0)] = acc[mine, place_rows(h, d, 0)] + got3[d, rows_in(h, RING)]
            for e in group:
                g2_copy(h, d, e).start()
            send_on(h, d, 0)

    def spread(h):
        for e in group:
            for d in dims:
                g2_copy(h, d, e).wait_recv()
                send_on(h, d, e)

    def hand_on(h, e):
        for d in dims:
            g1_copy(h, d, e % 2, e).wait_recv()
            gf_copy(h, d, e).start()

    def near_gathered(h):
        take(got1.at[:, :, rows_in(h)] if DIRECT[h] else far1.at[:, rows_in(h)], near_recv.at[h])

    def far_gathered(h):
        take(far1.at[:, rows_in(h)], far_recv.at[h])

    def update(chunk, first, count):
        right = stacked_halves(res, chunk, first, count)
        for b in range(blocks):
            rows = slice(b * own, (b + 1) * own)
            c_ref[chunk, rows] = c_ref[chunk, rows] - dot(w_ref[rows, 3 * first:3 * (first + count)], right)

    for first in range(0, depth, HALF):
        keep(vt.at[0], col, first, HALF)
    weigh(col)
    take(near.at[sibling], sib_recv)
    for first in range(0, depth, HALF):
        keep(vt.at[1], sibling, first, HALF)
    for i in range(0, chunks, 2):
        c_copy(i).wait()
        c_copy(i + 1).wait()
        near_job(order[i][1])
    for away in range(RING):
        prepare((away + 2) % RING)
    arrive(0)
    produce(0)
    last = len(PARTS) - 1
    if last == 2:
        arrive(1)
        produce(1)
    arrive(last)
    pass_on(0)
    produce(last)
    if last == 2 and not DIRECT[1]:
        pass_on(1)
    collect(0)
    if not DIRECT[last]:
        pass_on(last)
    weigh(sibling)
    weigh(across)
    if last == 2:
        collect(1)
    weigh(across_sibling)
    collect(2)
    pair(0)
    pair(1)
    pair(2)
    finish(0)
    finish(1)
    finish(2)
    spread(0)
    spread(1)
    for d in dims:
        update(chunk_of(d, 0), 0, HALF)
    for e in range(RING):
        hand_on(0, e)
    spread(last)
    if last == 2 and not DIRECT[1]:
        for e in range(RING):
            hand_on(1, e)
    if not DIRECT[last]:
        hand_on(last, 0)
    for d in dims:
        update(chunk_of(d, 0), HALF, HALF)
    near_gathered(0)
    if not DIRECT[last]:
        for e in range(1, RING):
            hand_on(last, e)
    for away in WAYS:
        for d in dims:
            update(chunk_of(d, away), 0, HALF)
    far_gathered(0)
    for h in range(1, len(PARTS)):
        near_gathered(h)
        far_gathered(h)

    take(near.at[pl.ds(0, 3)], send)
    for h in range(len(PARTS)):
        if DIRECT[h]:
            take(far1.at[:, rows_in(h)], send)
            for way in range(2):
                take(far1.at[:, rows_in(h)], send)
        else:
            take(passing.at[:, :, rows_in(h, 2)], send)
            take(got1.at[:, :, rows_in(h)], send)
        take(got2.at[:, :, rows_in(h, RING)], send)
        take(got3.at[:, rows_in(h, RING)], send)
        take(got2.at[:, :, rows_in(h, RING)], send)
        take(got1.at[:, :, rows_in(h)], send)
        take(far1.at[:, rows_in(h)], send)


def update_kernel(c_ref, w_ref, res, out_hbm, stage, sem):
    row = lax.axis_index("row")
    places = lax.rem(lax.div(row, 2), RING), lax.div(row, 2 * RING)
    chunks, height, width = c_ref.shape
    depth = res.shape[1]
    slots = stage.shape[0]
    pieces = 4
    size = height // pieces

    def chunk_of(i):
        d, away = lax.rem(i, 2), lax.div(i, 2)
        return d * RING + lax.rem(jnp.where(d == 0, places[0], places[1]) + jnp.where(away == 2, 3, jnp.where(away == 3, 2, away)), RING)

    def out_copy(i, ref, slot):
        lanes = pl.ds(pl.multiple_of(chunk_of(i) * width, width), width)
        return pltpu.make_async_copy(ref, out_hbm.at[:, lanes], sem.at[slot])

    for i in range(2):
        out_copy(i, c_ref.at[chunk_of(i)], slots + i).start()

    def step(i, carry, first):
        slot = lax.rem(i, slots)

        @pl.when(i >= slots + 2)
        def _():
            out_copy(i - slots, stage.at[slot], slot).wait()

        right = stacked_halves(res, chunk_of(i), first, depth - first)
        for p in range(pieces):
            rows = slice(p * size, (p + 1) * size)
            stage[slot, rows] = c_ref[chunk_of(i), rows] - dot(w_ref[rows, 3 * first:], right)
        out_copy(i, stage.at[slot], slot).start()
        return carry

    lax.fori_loop(2, 6, functools.partial(step, first=HALF), 0)
    lax.fori_loop(6, chunks, functools.partial(step, first=0), 0)
    for i in range(2):
        out_copy(i, c_ref.at[chunk_of(i)], slots + i).wait()
    for i in range(max(2, chunks - slots), chunks):
        out_copy(i, stage.at[i % slots], i % slots).wait()


def grid_shards(trailing, vectors, tfactor):
    height, columns = trailing.shape
    own, depth = vectors.shape
    chunks = 2 * RING
    width = columns // chunks
    blocks = height // own
    parts = len(PARTS)
    dma = pltpu.SemaphoreType.DMA
    vmem = pl.BlockSpec(memory_space=pltpu.VMEM)
    hbm = pl.BlockSpec(memory_space=pltpu.HBM)
    held, w_ref, res = pl.pallas_call(
        sum_kernel,
        out_shape=(
            pltpu.VMEM((chunks, height, width), F32),
            pltpu.VMEM((height, 3 * depth), BF16),
            pltpu.VMEM((chunks, depth, width), F32),
        ),
        in_specs=[hbm, hbm, hbm],
        out_specs=(vmem, vmem, vmem),
        scratch_shapes=[
            pltpu.VMEM((own, depth), F32),
            pltpu.VMEM((blocks, depth, own), F32),
            pltpu.VMEM((chunks, depth, width), F32),
            pltpu.VMEM((2, 2 * depth, own), BF16),
            pltpu.VMEM((2 * depth, 2 * own), BF16),
            pltpu.VMEM((RING, 2 * own, 2 * width), BF16),
            pltpu.VMEM((RING, 2 * own, 2 * width), BF16),
            pltpu.VMEM((2, 2, depth // 2, width), F32),
            pltpu.VMEM((2, 2, depth, width), F32),
            pltpu.VMEM((2, depth, width), F32),
            pltpu.VMEM((2, RING - 1, depth // RING, width), F32),
            pltpu.VMEM((2, depth // RING, width), F32),
            pltpu.VMEM((depth, depth), F32),
            dma((chunks,)), dma((2,)),
            dma, dma, dma((parts, V_PIECES)), dma((parts,)),
            dma((parts, 2, 2)), dma((parts, 2)), dma((parts, 2)), dma((parts, 2)),
            dma((parts, 2, RING)), dma((parts, 2, RING)), dma((parts,)), dma((parts,)),
        ],
        compiler_params=pltpu.CompilerParams(
            collective_id=0, has_side_effects=True, vmem_limit_bytes=42 << 20
        ),
    )(trailing, vectors, tfactor)
    slots = 4
    return pl.pallas_call(
        update_kernel,
        out_shape=jax.ShapeDtypeStruct((height, columns), F32),
        in_specs=[vmem, vmem, vmem],
        out_specs=hbm,
        scratch_shapes=[pltpu.VMEM((slots, height, width), F32), dma((slots + 2,))],
        compiler_params=pltpu.CompilerParams(vmem_limit_bytes=20 << 20),
    )(held, w_ref, res)


def plain_shards(trailing, vectors, tfactor):
    dot = functools.partial(jnp.dot, precision=lax.Precision.HIGH, preferred_element_type=F32)
    near_vectors = lax.all_gather(vectors, "col", axis=0, tiled=True)
    summed = lax.psum(dot(near_vectors.T, trailing), "row")
    return trailing - dot(near_vectors, dot(tfactor, summed))


def solution(mesh):
    placed = (P("row", "col"), P(("row", "col"), None), P())
    fits = mesh.shape["row"] == 2 * RING * RING and mesh.shape["col"] == 4

    def shards(trailing, vectors, tfactor):
        if fits and trailing.shape == (2048, 2048) and vectors.shape == (512, 256):
            return grid_shards(trailing, vectors, tfactor)
        return plain_shards(trailing, vectors, tfactor)

    return jax.shard_map(
        shards, mesh=mesh, in_specs=placed, out_specs=P("row", "col"), check_vma=False
    )
```

```python
import functools

import jax
import jax.numpy as jnp
from jax import lax
from jax.experimental import pallas as pl
from jax.experimental.pallas import tpu as pltpu
from jax.sharding import PartitionSpec as P

MESH = pl.DeviceIdType.MESH
F32, BF16 = jnp.float32, jnp.bfloat16
RING = 4
HALF = 128
PARTS = ((0, 128), (128, 64), (192, 64))
DIRECT = (False, False, True)
V_PIECES = 2
WAYS = (1, -1)
OTHERS = (0, 1, -1, 2)


def split(x):
    high = x.astype(BF16)
    return high, (x - high.astype(F32)).astype(BF16)


def dot(a, b):
    return jnp.dot(a, b, preferred_element_type=F32)


def dot3(a_high, a_low, b_high, b_low):
    return dot(a_high, b_high) + (dot(a_low, b_high) + dot(a_high, b_low))


def stacked_halves(ref, chunk, first, count):
    rows = []
    for at in range(first, first + count, HALF):
        high, low = split(ref[chunk, at:at + HALF])
        rows += [high, high, low]
    return jnp.concatenate(rows, axis=0)


def sum_kernel(
    c_hbm, v_hbm, t_hbm, c_ref, w_ref, res,
    v_ref, near, acc, vt, vt_far, c_high, c_low, passing, got1, far1, got2, got3, t_ref, c_sem, l_sem,
    send, sib_recv, v_recv, f_recv, a_recv, r1_recv, r2_recv, y_recv, g2_recv, g1_recv, near_recv, far_recv,
):
    row, col = lax.axis_index("row"), lax.axis_index("col")
    core, y_hi = lax.rem(col, 2), lax.div(col, 2)
    z, x, y_lo = lax.div(row, 2 * RING), lax.rem(lax.div(row, 2), RING), lax.rem(row, 2)
    sibling = y_hi * 2 + (1 - core)
    across = (1 - y_hi) * 2 + core
    across_sibling = (1 - y_hi) * 2 + (1 - core)
    blocks, depth, own = near.shape
    chunks, height, width = c_ref.shape
    group = range(1, RING)
    dims = range(2)
    pos, other = (x, z), (z, x)

    def wrap(i):
        return lax.rem(i + RING, RING)

    def target(d, away, across_other, flip):
        first = wrap(pos[d] + away)
        second = wrap(other[d] + across_other)
        zz, xx = (second, first) if d == 0 else (first, second)
        return (zz * (2 * RING) + xx * 2 + lax.rem(y_lo + flip, 2), col)

    def remote(src, dst, recv, to):
        return pltpu.make_async_remote_copy(
            src_ref=src, dst_ref=dst, send_sem=send, recv_sem=recv, device_id=to, device_id_type=MESH
        )

    def take(ref, sem):
        pltpu.make_async_copy(ref, ref, sem).wait()

    def chunk_of(d, away):
        return d * RING + wrap(pos[d] + away)

    order = [(d, away) for away in (2, 1, -1, 0) for d in dims]

    def c_copy(i):
        chunk = chunk_of(*order[i])
        return pltpu.make_async_copy(
            c_hbm.at[:, pl.ds(pl.multiple_of(chunk * width, width), width)], c_ref.at[chunk], c_sem.at[i]
        )

    v_copy = pltpu.make_async_copy(v_hbm, v_ref, l_sem.at[0])
    t_copy = pltpu.make_async_copy(t_hbm, t_ref, l_sem.at[1])
    v_copy.start()
    t_copy.start()

    barrier = pltpu.get_barrier_semaphore()
    friends = [(row, sibling), (row, across)]
    friends += [target(d, away, 0, 0) for d in dims for away in (1, -1, 2)]
    friends += [target(0, 0, 0, 1)]
    for friend in friends:
        pl.semaphore_signal(barrier, inc=1, device_id=friend, device_id_type=MESH)
    v_copy.wait()
    t_copy.wait()
    for i in range(chunks):
        c_copy(i).start()
    pl.semaphore_wait(barrier, len(friends))

    def rows_in(h, share=1, place=0):
        first, count = PARTS[h]
        return pl.ds(pl.multiple_of(first // share + place * (count // share), 8), count // share)

    def v_copy_across(h, p):
        size = own // V_PIECES
        there = near.at[col, rows_in(h), pl.ds(p * size, size)]
        return remote(there, there, v_recv.at[h, p], (row, across))

    def forward(h, p):
        size = own // V_PIECES
        there = near.at[across, rows_in(h), pl.ds(p * size, size)]
        return remote(there, there, f_recv.at[h], (row, sibling))

    for h, (first, count) in enumerate(PARTS):
        for at in range(-(-first // HALF) * HALF, first + count, HALF):
            near[col, at:at + HALF] = v_ref[:, at:at + HALF].T
        for p in range(V_PIECES):
            v_copy_across(h, p).start()
    sib = remote(near.at[col], near.at[col], sib_recv, (row, sibling))
    sib.start()

    def keep(ref, block, first, count, lanes=slice(None)):
        high, low = split(near[block, first:first + count])
        ref[2 * first:2 * first + count, lanes] = high
        ref[2 * first + count:2 * (first + count), lanes] = low

    def arrive(h):
        for p in range(V_PIECES):
            v_copy_across(h, p).wait_recv()
            forward(h, p).start()
        keep(vt_far, across, *PARTS[h], slice(0, own))

    def arrive_sibling(h):
        take(near.at[across_sibling, rows_in(h)], f_recv.at[h])
        keep(vt_far, across_sibling, *PARTS[h], slice(own, 2 * own))

    def product(ref, first, count, high, low):
        both = dot(ref[2 * first:2 * (first + count)], high)
        return both[:count] + (both[count:] + dot(ref[2 * first:2 * first + count], low))

    def piece(away, block):
        rows = pl.ds(pl.multiple_of(block * own, own), own)
        return split(jnp.concatenate([c_ref[chunk_of(d, away), rows] for d in dims], axis=1))

    def near_job(away):
        c0, c1 = piece(away, col), piece(away, sibling)
        for first in range(0, depth, HALF):
            total = product(vt.at[0], first, HALF, *c0) + product(vt.at[1], first, HALF, *c1)
            for d in dims:
                acc[chunk_of(d, away), first:first + HALF] = total[:, d * width:(d + 1) * width]

    def prepare(away):
        for i, block in enumerate((across, across_sibling)):
            c_high[away, i * own:(i + 1) * own], c_low[away, i * own:(i + 1) * own] = piece(away, block)

    def job(away, h, which=slice(None)):
        first, count = PARTS[h]
        total = product(vt_far.at[:, which], first, count, c_high[away, which], c_low[away, which])
        for d in dims:
            acc[chunk_of(d, away), first:first + count] += total[:, d * width:(d + 1) * width]

    def weigh(block):
        t_high, t_low = split(t_ref[...].T)
        high, low = split(near[block])
        high, low = split(dot3(t_high, t_low, high, low).T)
        rows = pl.ds(pl.multiple_of(block * own, own), own)
        for first in range(0, depth, HALF):
            lanes = slice(first, first + HALF)
            w_ref[rows, 3 * first:3 * first + HALF] = high[:, lanes]
            w_ref[rows, 3 * first + HALF:3 * first + 2 * HALF] = low[:, lanes]
            w_ref[rows, 3 * first + 2 * HALF:3 * (first + HALF)] = high[:, lanes]

    def half_rows(h, way):
        first, count = PARTS[h]
        return pl.ds(first + way * (count // 2), count // 2)

    def upper(h, way):
        return half_rows(h, way)

    def lower(h, way):
        return half_rows(h, 1 - way)

    def a_copy(h, d, way):
        return remote(
            acc.at[chunk_of(d, 2), upper(h, way)], passing.at[d, way, rows_in(h, 2)],
            a_recv.at[h, d, way], target(d, WAYS[way], 0, 0),
        )

    def b_copy(h, d, way):
        rows = rows_in(h) if DIRECT[h] else lower(h, way)
        return remote(
            acc.at[chunk_of(d, WAYS[way]), rows], got1.at[d, way, rows], r1_recv.at[h, d], target(d, WAYS[way], 0, 0)
        )

    def s_copy(h, d, way):
        rows = upper(h, way)
        return remote(
            acc.at[chunk_of(d, WAYS[way]), rows], got1.at[d, way, rows], r1_recv.at[h, d], target(d, WAYS[way], 0, 0)
        )

    def far_copy(h, d):
        return remote(
            acc.at[chunk_of(d, 2), rows_in(h)], far1.at[d, rows_in(h)], a_recv.at[h, d, 0], target(d, 2, 0, 0)
        )

    def place_rows(h, d, away):
        first, count = PARTS[h]
        sub = count // RING
        return pl.ds(pl.multiple_of(first + wrap(other[d] + away) * sub, sub), sub)

    def r2_copy(h, d, e):
        return remote(
            acc.at[chunk_of(d, 0), place_rows(h, d, OTHERS[e])], got2.at[d, e - 1, rows_in(h, RING)], r2_recv.at[h, d],
            target(d, 0, OTHERS[e], 0),
        )

    def y_copy(h, d):
        return remote(
            acc.at[chunk_of(d, 0), place_rows(h, d, 0)], got3.at[d, rows_in(h, RING)], y_recv.at[h, d],
            target(d, 0, 0, 1),
        )

    def g2_copy(h, d, e):
        ref = res.at[chunk_of(d, 0), place_rows(h, d, 0)]
        return remote(ref, ref, g2_recv.at[h, d, e], target(d, 0, OTHERS[e], 0))

    def g1_copy(h, d, way, e):
        ref = res.at[chunk_of(d, 0), place_rows(h, d, -OTHERS[e])]
        recv = g1_recv.at[h, d, e] if way == e % 2 and not DIRECT[h] else near_recv.at[h]
        return remote(ref, ref, recv, target(d, WAYS[way], 0, 0))

    def gf_copy(h, d, e):
        way = e % 2
        chunk = chunk_of(d, 0) if DIRECT[h] else chunk_of(d, -WAYS[way])
        ref = res.at[chunk, place_rows(h, d, -OTHERS[e])]
        return remote(ref, ref, far_recv.at[h], target(d, 2 if DIRECT[h] else WAYS[way], 0, 0))

    def produce(h):
        job(2, h, slice(0, own))
        arrive_sibling(h)
        job(2, h, slice(own, 2 * own))
        for d in dims:
            if DIRECT[h]:
                far_copy(h, d).start()
            else:
                for way in range(2):
                    a_copy(h, d, way).start()
        for way in range(2):
            job(WAYS[way] % RING, h)
            for d in dims:
                b_copy(h, d, way).start()
        job(0, h)

    def pass_on(h):
        for d in dims:
            for way in range(2):
                a_copy(h, d, way).wait_recv()
                acc[chunk_of(d, WAYS[way]), upper(h, way)] += passing[d, way, rows_in(h, 2)]
                s_copy(h, d, way).start()

    def collect(h):
        rows = rows_in(h)
        for d in dims:
            take(got1.at[d, :, rows], r1_recv.at[h, d])
            total = got1[d, 0, rows] + got1[d, 1, rows]
            if DIRECT[h]:
                take(far1.at[d, rows], a_recv.at[h, d, 0])
                total += far1[d, rows]
            acc[chunk_of(d, 0), rows] += total
            for e in group:
                r2_copy(h, d, e).start()

    def pair(h):
        rows = rows_in(h, RING)
        for d in dims:
            take(got2.at[d, :, rows], r2_recv.at[h, d])
            acc[chunk_of(d, 0), place_rows(h, d, 0)] += got2[d, 0, rows] + (got2[d, 1, rows] + got2[d, 2, rows])
            y_copy(h, d).start()

    def send_on(h, d, e):
        if DIRECT[h]:
            gf_copy(h, d, e).start()
        for way in range(2):
            g1_copy(h, d, way, e).start()

    def finish(h):
        for d in dims:
            mine = chunk_of(d, 0)
            y_copy(h, d).wait_recv()
            res[mine, place_rows(h, d, 0)] = acc[mine, place_rows(h, d, 0)] + got3[d, rows_in(h, RING)]
            for e in group:
                g2_copy(h, d, e).start()
            send_on(h, d, 0)

    def spread(h):
        for e in group:
            for d in dims:
                g2_copy(h, d, e).wait_recv()
                send_on(h, d, e)

    def hand_on(h, e):
        for d in dims:
            g1_copy(h, d, e % 2, e).wait_recv()
            gf_copy(h, d, e).start()

    def near_gathered(h):
        take(got1.at[:, :, rows_in(h)] if DIRECT[h] else far1.at[:, rows_in(h)], near_recv.at[h])

    def far_gathered(h):
        take(far1.at[:, rows_in(h)], far_recv.at[h])

    def update(chunk, first, count):
        right = stacked_halves(res, chunk, first, count)
        for b in range(blocks):
            rows = slice(b * own, (b + 1) * own)
            c_ref[chunk, rows] = c_ref[chunk, rows] - dot(w_ref[rows, 3 * first:3 * (first + count)], right)

    for first in range(0, depth, HALF):
        keep(vt.at[0], col, first, HALF)
    weigh(col)
    take(near.at[sibling], sib_recv)
    for first in range(0, depth, HALF):
        keep(vt.at[1], sibling, first, HALF)
    for i in range(0, chunks, 2):
        c_copy(i).wait()
        c_copy(i + 1).wait()
        near_job(order[i][1])
    for away in range(RING):
        prepare((away + 2) % RING)
    arrive(0)
    produce(0)
    last = len(PARTS) - 1
    if last == 2:
        arrive(1)
        produce(1)
    arrive(last)
    pass_on(0)
    produce(last)
    if last == 2 and not DIRECT[1]:
        pass_on(1)
    weigh(sibling)
    weigh(across)
    collect(0)
    if not DIRECT[last]:
        pass_on(last)
    weigh(across_sibling)
    collect(1)
    collect(2)
    pair(0)
    pair(1)
    pair(2)
    finish(0)
    finish(1)
    finish(2)
    spread(0)
    spread(1)
    for d in dims:
        update(chunk_of(d, 0), 0, HALF)
    for e in range(RING):
        hand_on(0, e)
    spread(last)
    if last == 2 and not DIRECT[1]:
        for e in range(RING):
            hand_on(1, e)
    if not DIRECT[last]:
        hand_on(last, 0)
    for d in dims:
        update(chunk_of(d, 0), HALF, HALF)
    near_gathered(0)
    if not DIRECT[last]:
        for e in range(1, RING):
            hand_on(last, e)
    for away in WAYS:
        for d in dims:
            update(chunk_of(d, away), 0, HALF)
    far_gathered(0)
    for h in range(1, len(PARTS)):
        near_gathered(h)
        far_gathered(h)

    take(near.at[pl.ds(0, 3)], send)
    for h in range(len(PARTS)):
        if DIRECT[h]:
            take(far1.at[:, rows_in(h)], send)
            for way in range(2):
                take(far1.at[:, rows_in(h)], send)
        else:
            take(passing.at[:, :, rows_in(h, 2)], send)
            take(got1.at[:, :, rows_in(h)], send)
        take(got2.at[:, :, rows_in(h, RING)], send)
        take(got3.at[:, rows_in(h, RING)], send)
        take(got2.at[:, :, rows_in(h, RING)], send)
        take(got1.at[:, :, rows_in(h)], send)
        take(far1.at[:, rows_in(h)], send)


def update_kernel(c_ref, w_ref, res, out_hbm, stage, sem):
    row = lax.axis_index("row")
    places = lax.rem(lax.div(row, 2), RING), lax.div(row, 2 * RING)
    chunks, height, width = c_ref.shape
    depth = res.shape[1]
    slots = stage.shape[0]
    pieces = 4
    size = height // pieces

    def chunk_of(i):
        d, away = lax.rem(i, 2), lax.div(i, 2)
        return d * RING + lax.rem(jnp.where(d == 0, places[0], places[1]) + jnp.where(away == 2, 3, jnp.where(away == 3, 2, away)), RING)

    def out_copy(i, ref, slot):
        lanes = pl.ds(pl.multiple_of(chunk_of(i) * width, width), width)
        return pltpu.make_async_copy(ref, out_hbm.at[:, lanes], sem.at[slot])

    for i in range(2):
        out_copy(i, c_ref.at[chunk_of(i)], slots + i).start()

    def step(i, carry, first):
        slot = lax.rem(i, slots)

        @pl.when(i >= slots + 2)
        def _():
            out_copy(i - slots, stage.at[slot], slot).wait()

        right = stacked_halves(res, chunk_of(i), first, depth - first)
        for p in range(pieces):
            rows = slice(p * size, (p + 1) * size)
            stage[slot, rows] = c_ref[chunk_of(i), rows] - dot(w_ref[rows, 3 * first:], right)
        out_copy(i, stage.at[slot], slot).start()
        return carry

    lax.fori_loop(2, 6, functools.partial(step, first=HALF), 0)
    lax.fori_loop(6, chunks, functools.partial(step, first=0), 0)
    for i in range(2):
        out_copy(i, c_ref.at[chunk_of(i)], slots + i).wait()
    for i in range(max(2, chunks - slots), chunks):
        out_copy(i, stage.at[i % slots], i % slots).wait()


def grid_shards(trailing, vectors, tfactor):
    height, columns = trailing.shape
    own, depth = vectors.shape
    chunks = 2 * RING
    width = columns // chunks
    blocks = height // own
    parts = len(PARTS)
    dma = pltpu.SemaphoreType.DMA
    vmem = pl.BlockSpec(memory_space=pltpu.VMEM)
    hbm = pl.BlockSpec(memory_space=pltpu.HBM)
    held, w_ref, res = pl.pallas_call(
        sum_kernel,
        out_shape=(
            pltpu.VMEM((chunks, height, width), F32),
            pltpu.VMEM((height, 3 * depth), BF16),
            pltpu.VMEM((chunks, depth, width), F32),
        ),
        in_specs=[hbm, hbm, hbm],
        out_specs=(vmem, vmem, vmem),
        scratch_shapes=[
            pltpu.VMEM((own, depth), F32),
            pltpu.VMEM((blocks, depth, own), F32),
            pltpu.VMEM((chunks, depth, width), F32),
            pltpu.VMEM((2, 2 * depth, own), BF16),
            pltpu.VMEM((2 * depth, 2 * own), BF16),
            pltpu.VMEM((RING, 2 * own, 2 * width), BF16),
            pltpu.VMEM((RING, 2 * own, 2 * width), BF16),
            pltpu.VMEM((2, 2, depth // 2, width), F32),
            pltpu.VMEM((2, 2, depth, width), F32),
            pltpu.VMEM((2, depth, width), F32),
            pltpu.VMEM((2, RING - 1, depth // RING, width), F32),
            pltpu.VMEM((2, depth // RING, width), F32),
            pltpu.VMEM((depth, depth), F32),
            dma((chunks,)), dma((2,)),
            dma, dma, dma((parts, V_PIECES)), dma((parts,)),
            dma((parts, 2, 2)), dma((parts, 2)), dma((parts, 2)), dma((parts, 2)),
            dma((parts, 2, RING)), dma((parts, 2, RING)), dma((parts,)), dma((parts,)),
        ],
        compiler_params=pltpu.CompilerParams(
            collective_id=0, has_side_effects=True, vmem_limit_bytes=42 << 20
        ),
    )(trailing, vectors, tfactor)
    slots = 4
    return pl.pallas_call(
        update_kernel,
        out_shape=jax.ShapeDtypeStruct((height, columns), F32),
        in_specs=[vmem, vmem, vmem],
        out_specs=hbm,
        scratch_shapes=[pltpu.VMEM((slots, height, width), F32), dma((slots + 2,))],
        compiler_params=pltpu.CompilerParams(vmem_limit_bytes=20 << 20),
    )(held, w_ref, res)


def plain_shards(trailing, vectors, tfactor):
    dot = functools.partial(jnp.dot, precision=lax.Precision.HIGH, preferred_element_type=F32)
    near_vectors = lax.all_gather(vectors, "col", axis=0, tiled=True)
    summed = lax.psum(dot(near_vectors.T, trailing), "row")
    return trailing - dot(near_vectors, dot(tfactor, summed))


def solution(mesh):
    placed = (P("row", "col"), P(("row", "col"), None), P())
    fits = mesh.shape["row"] == 2 * RING * RING and mesh.shape["col"] == 4

    def shards(trailing, vectors, tfactor):
        if fits and trailing.shape == (2048, 2048) and vectors.shape == (512, 256):
            return grid_shards(trailing, vectors, tfactor)
        return plain_shards(trailing, vectors, tfactor)

    return jax.shard_map(
        shards, mesh=mesh, in_specs=placed, out_specs=P("row", "col"), check_vma=False
    )
```

```python
import functools

import jax
import jax.numpy as jnp
from jax import lax
from jax.experimental import pallas as pl
from jax.experimental.pallas import tpu as pltpu
from jax.sharding import PartitionSpec as P

MESH = pl.DeviceIdType.MESH
F32, BF16 = jnp.float32, jnp.bfloat16
RING = 4
HALF = 128
PARTS = ((0, 128), (128, 64), (192, 64))
DIRECT = (False, False, True)
V_PIECES = 2
WAYS = (1, -1)
OTHERS = (0, 1, -1, 2)


def split(x):
    high = x.astype(BF16)
    return high, (x - high.astype(F32)).astype(BF16)


def dot(a, b):
    return jnp.dot(a, b, preferred_element_type=F32)


def dot3(a_high, a_low, b_high, b_low):
    return dot(a_high, b_high) + (dot(a_low, b_high) + dot(a_high, b_low))


def stacked_halves(ref, chunk, first, count):
    rows = []
    for at in range(first, first + count, HALF):
        high, low = split(ref[chunk, at:at + HALF])
        rows += [high, high, low]
    return jnp.concatenate(rows, axis=0)


def sum_kernel(
    c_hbm, v_hbm, t_hbm, c_ref, w_ref, res,
    v_ref, near, acc, vt, vt_far, c_high, c_low, passing, got1, far1, got2, got3, t_ref, c_sem, l_sem,
    send, sib_recv, v_recv, f_recv, a_recv, r1_recv, r2_recv, y_recv, g2_recv, g1_recv, near_recv, far_recv,
):
    row, col = lax.axis_index("row"), lax.axis_index("col")
    core, y_hi = lax.rem(col, 2), lax.div(col, 2)
    z, x, y_lo = lax.div(row, 2 * RING), lax.rem(lax.div(row, 2), RING), lax.rem(row, 2)
    sibling = y_hi * 2 + (1 - core)
    across = (1 - y_hi) * 2 + core
    across_sibling = (1 - y_hi) * 2 + (1 - core)
    blocks, depth, own = near.shape
    chunks, height, width = c_ref.shape
    group = range(1, RING)
    dims = range(2)
    pos, other = (x, z), (z, x)

    def wrap(i):
        return lax.rem(i + RING, RING)

    def target(d, away, across_other, flip):
        first = wrap(pos[d] + away)
        second = wrap(other[d] + across_other)
        zz, xx = (second, first) if d == 0 else (first, second)
        return (zz * (2 * RING) + xx * 2 + lax.rem(y_lo + flip, 2), col)

    def remote(src, dst, recv, to):
        return pltpu.make_async_remote_copy(
            src_ref=src, dst_ref=dst, send_sem=send, recv_sem=recv, device_id=to, device_id_type=MESH
        )

    def take(ref, sem):
        pltpu.make_async_copy(ref, ref, sem).wait()

    def chunk_of(d, away):
        return d * RING + wrap(pos[d] + away)

    order = [(d, away) for away in (2, 1, -1, 0) for d in dims]

    def c_copy(i):
        chunk = chunk_of(*order[i])
        return pltpu.make_async_copy(
            c_hbm.at[:, pl.ds(pl.multiple_of(chunk * width, width), width)], c_ref.at[chunk], c_sem.at[i]
        )

    v_copy = pltpu.make_async_copy(v_hbm, v_ref, l_sem.at[0])
    t_copy = pltpu.make_async_copy(t_hbm, t_ref, l_sem.at[1])
    v_copy.start()
    t_copy.start()

    barrier = pltpu.get_barrier_semaphore()
    friends = [(row, sibling), (row, across)]
    friends += [target(d, away, 0, 0) for d in dims for away in (1, -1, 2)]
    friends += [target(0, 0, 0, 1)]
    for friend in friends:
        pl.semaphore_signal(barrier, inc=1, device_id=friend, device_id_type=MESH)
    v_copy.wait()
    t_copy.wait()
    for i in range(chunks):
        c_copy(i).start()
    pl.semaphore_wait(barrier, len(friends))

    def rows_in(h, share=1, place=0):
        first, count = PARTS[h]
        return pl.ds(pl.multiple_of(first // share + place * (count // share), 8), count // share)

    def v_copy_across(h, p):
        size = own // V_PIECES
        there = near.at[col, rows_in(h), pl.ds(p * size, size)]
        return remote(there, there, v_recv.at[h, p], (row, across))

    def forward(h, p):
        size = own // V_PIECES
        there = near.at[across, rows_in(h), pl.ds(p * size, size)]
        return remote(there, there, f_recv.at[h], (row, sibling))

    for h, (first, count) in enumerate(PARTS):
        for at in range(-(-first // HALF) * HALF, first + count, HALF):
            near[col, at:at + HALF] = v_ref[:, at:at + HALF].T
        for p in range(V_PIECES):
            v_copy_across(h, p).start()
    sib = remote(near.at[col], near.at[col], sib_recv, (row, sibling))
    sib.start()

    def keep(ref, block, first, count, lanes=slice(None)):
        high, low = split(near[block, first:first + count])
        ref[2 * first:2 * first + count, lanes] = high
        ref[2 * first + count:2 * (first + count), lanes] = low

    def arrive(h):
        for p in range(V_PIECES):
            v_copy_across(h, p).wait_recv()
            forward(h, p).start()
        keep(vt_far, across, *PARTS[h], slice(0, own))

    def arrive_sibling(h):
        take(near.at[across_sibling, rows_in(h)], f_recv.at[h])
        keep(vt_far, across_sibling, *PARTS[h], slice(own, 2 * own))

    def product(ref, first, count, high, low):
        both = dot(ref[2 * first:2 * (first + count)], high)
        return both[:count] + (both[count:] + dot(ref[2 * first:2 * first + count], low))

    def piece(away, block):
        rows = pl.ds(pl.multiple_of(block * own, own), own)
        return split(jnp.concatenate([c_ref[chunk_of(d, away), rows] for d in dims], axis=1))

    def near_job(away):
        c0, c1 = piece(away, col), piece(away, sibling)
        for first in range(0, depth, HALF):
            total = product(vt.at[0], first, HALF, *c0) + product(vt.at[1], first, HALF, *c1)
            for d in dims:
                acc[chunk_of(d, away), first:first + HALF] = total[:, d * width:(d + 1) * width]

    def prepare(away):
        for i, block in enumerate((across, across_sibling)):
            c_high[away, i * own:(i + 1) * own], c_low[away, i * own:(i + 1) * own] = piece(away, block)

    def job(away, h, which=slice(None)):
        first, count = PARTS[h]
        total = product(vt_far.at[:, which], first, count, c_high[away, which], c_low[away, which])
        for d in dims:
            acc[chunk_of(d, away), first:first + count] += total[:, d * width:(d + 1) * width]

    def weigh(block):
        t_high, t_low = split(t_ref[...].T)
        high, low = split(near[block])
        high, low = split(dot3(t_high, t_low, high, low).T)
        rows = pl.ds(pl.multiple_of(block * own, own), own)
        for first in range(0, depth, HALF):
            lanes = slice(first, first + HALF)
            w_ref[rows, 3 * first:3 * first + HALF] = high[:, lanes]
            w_ref[rows, 3 * first + HALF:3 * first + 2 * HALF] = low[:, lanes]
            w_ref[rows, 3 * first + 2 * HALF:3 * (first + HALF)] = high[:, lanes]

    def half_rows(h, way):
        first, count = PARTS[h]
        return pl.ds(first + way * (count // 2), count // 2)

    def upper(h, way):
        return half_rows(h, way)

    def lower(h, way):
        return half_rows(h, 1 - way)

    def a_copy(h, d, way):
        return remote(
            acc.at[chunk_of(d, 2), upper(h, way)], passing.at[d, way, rows_in(h, 2)],
            a_recv.at[h, d, way], target(d, WAYS[way], 0, 0),
        )

    def b_copy(h, d, way):
        rows = rows_in(h) if DIRECT[h] else lower(h, way)
        return remote(
            acc.at[chunk_of(d, WAYS[way]), rows], got1.at[d, way, rows], r1_recv.at[h, d], target(d, WAYS[way], 0, 0)
        )

    def s_copy(h, d, way):
        rows = upper(h, way)
        return remote(
            acc.at[chunk_of(d, WAYS[way]), rows], got1.at[d, way, rows], r1_recv.at[h, d], target(d, WAYS[way], 0, 0)
        )

    def far_copy(h, d):
        return remote(
            acc.at[chunk_of(d, 2), rows_in(h)], far1.at[d, rows_in(h)], a_recv.at[h, d, 0], target(d, 2, 0, 0)
        )

    def place_rows(h, d, away):
        first, count = PARTS[h]
        sub = count // RING
        return pl.ds(pl.multiple_of(first + wrap(other[d] + away) * sub, sub), sub)

    def r2_copy(h, d, e):
        return remote(
            acc.at[chunk_of(d, 0), place_rows(h, d, OTHERS[e])], got2.at[d, e - 1, rows_in(h, RING)], r2_recv.at[h, d],
            target(d, 0, OTHERS[e], 0),
        )

    def y_copy(h, d):
        return remote(
            acc.at[chunk_of(d, 0), place_rows(h, d, 0)], got3.at[d, rows_in(h, RING)], y_recv.at[h, d],
            target(d, 0, 0, 1),
        )

    def g2_copy(h, d, e):
        ref = res.at[chunk_of(d, 0), place_rows(h, d, 0)]
        return remote(ref, ref, g2_recv.at[h, d, e], target(d, 0, OTHERS[e], 0))

    def g1_copy(h, d, way, e):
        ref = res.at[chunk_of(d, 0), place_rows(h, d, -OTHERS[e])]
        recv = g1_recv.at[h, d, e] if way == e % 2 and not DIRECT[h] else near_recv.at[h]
        return remote(ref, ref, recv, target(d, WAYS[way], 0, 0))

    def gf_copy(h, d, e):
        way = e % 2
        chunk = chunk_of(d, 0) if DIRECT[h] else chunk_of(d, -WAYS[way])
        ref = res.at[chunk, place_rows(h, d, -OTHERS[e])]
        return remote(ref, ref, far_recv.at[h], target(d, 2 if DIRECT[h] else WAYS[way], 0, 0))

    def produce(h):
        job(2, h, slice(0, own))
        arrive_sibling(h)
        job(2, h, slice(own, 2 * own))
        for d in dims:
            if DIRECT[h]:
                far_copy(h, d).start()
            else:
                for way in range(2):
                    a_copy(h, d, way).start()
        for way in range(2):
            job(WAYS[way] % RING, h)
            for d in dims:
                b_copy(h, d, way).start()
        job(0, h)

    def pass_on(h):
        for d in dims:
            for way in range(2):
                a_copy(h, d, way).wait_recv()
                acc[chunk_of(d, WAYS[way]), upper(h, way)] += passing[d, way, rows_in(h, 2)]
                s_copy(h, d, way).start()

    def collect(h):
        rows = rows_in(h)
        for d in dims:
            take(got1.at[d, :, rows], r1_recv.at[h, d])
            total = got1[d, 0, rows] + got1[d, 1, rows]
            if DIRECT[h]:
                take(far1.at[d, rows], a_recv.at[h, d, 0])
                total += far1[d, rows]
            acc[chunk_of(d, 0), rows] += total
            for e in group:
                r2_copy(h, d, e).start()

    def pair(h):
        rows = rows_in(h, RING)
        for d in dims:
            take(got2.at[d, :, rows], r2_recv.at[h, d])
            acc[chunk_of(d, 0), place_rows(h, d, 0)] += got2[d, 0, rows] + (got2[d, 1, rows] + got2[d, 2, rows])
            y_copy(h, d).start()

    def send_on(h, d, e):
        if DIRECT[h]:
            gf_copy(h, d, e).start()
        for way in range(2):
            g1_copy(h, d, way, e).start()

    def finish(h):
        for d in dims:
            mine = chunk_of(d, 0)
            y_copy(h, d).wait_recv()
            res[mine, place_rows(h, d, 0)] = acc[mine, place_rows(h, d, 0)] + got3[d, rows_in(h, RING)]
            for e in group:
                g2_copy(h, d, e).start()
            send_on(h, d, 0)

    def spread(h):
        for e in group:
            for d in dims:
                g2_copy(h, d, e).wait_recv()
                send_on(h, d, e)

    def hand_on(h, e):
        for d in dims:
            g1_copy(h, d, e % 2, e).wait_recv()
            gf_copy(h, d, e).start()

    def near_gathered(h):
        take(got1.at[:, :, rows_in(h)] if DIRECT[h] else far1.at[:, rows_in(h)], near_recv.at[h])

    def far_gathered(h):
        take(far1.at[:, rows_in(h)], far_recv.at[h])

    def update(chunk, first, count):
        right = stacked_halves(res, chunk, first, count)
        for b in range(blocks):
            rows = slice(b * own, (b + 1) * own)
            c_ref[chunk, rows] = c_ref[chunk, rows] - dot(w_ref[rows, 3 * first:3 * (first + count)], right)

    for first in range(0, depth, HALF):
        keep(vt.at[0], col, first, HALF)
    weigh(col)
    take(near.at[sibling], sib_recv)
    for first in range(0, depth, HALF):
        keep(vt.at[1], sibling, first, HALF)
    for i in range(0, chunks, 2):
        c_copy(i).wait()
        c_copy(i + 1).wait()
        near_job(order[i][1])
    for away in range(RING):
        prepare((away + 2) % RING)
    arrive(0)
    produce(0)
    last = len(PARTS) - 1
    if last == 2:
        arrive(1)
        produce(1)
    arrive(last)
    pass_on(0)
    produce(last)
    if last == 2 and not DIRECT[1]:
        pass_on(1)
    weigh(sibling)
    weigh(across)
    collect(0)
    if not DIRECT[last]:
        pass_on(last)
    weigh(across_sibling)
    collect(2)
    collect(1)
    pair(0)
    pair(1)
    pair(2)
    finish(0)
    finish(1)
    finish(2)
    spread(0)
    spread(1)
    for d in dims:
        update(chunk_of(d, 0), 0, HALF)
    for e in range(RING):
        hand_on(0, e)
    spread(last)
    if last == 2 and not DIRECT[1]:
        for e in range(RING):
            hand_on(1, e)
    if not DIRECT[last]:
        hand_on(last, 0)
    for d in dims:
        update(chunk_of(d, 0), HALF, HALF)
    near_gathered(0)
    if not DIRECT[last]:
        for e in range(1, RING):
            hand_on(last, e)
    for away in WAYS:
        for d in dims:
            update(chunk_of(d, away), 0, HALF)
    far_gathered(0)
    for h in range(1, len(PARTS)):
        near_gathered(h)
        far_gathered(h)

    take(near.at[pl.ds(0, 3)], send)
    for h in range(len(PARTS)):
        if DIRECT[h]:
            take(far1.at[:, rows_in(h)], send)
            for way in range(2):
                take(far1.at[:, rows_in(h)], send)
        else:
            take(passing.at[:, :, rows_in(h, 2)], send)
            take(got1.at[:, :, rows_in(h)], send)
        take(got2.at[:, :, rows_in(h, RING)], send)
        take(got3.at[:, rows_in(h, RING)], send)
        take(got2.at[:, :, rows_in(h, RING)], send)
        take(got1.at[:, :, rows_in(h)], send)
        take(far1.at[:, rows_in(h)], send)


def update_kernel(c_ref, w_ref, res, out_hbm, stage, sem):
    row = lax.axis_index("row")
    places = lax.rem(lax.div(row, 2), RING), lax.div(row, 2 * RING)
    chunks, height, width = c_ref.shape
    depth = res.shape[1]
    slots = stage.shape[0]
    pieces = 4
    size = height // pieces

    def chunk_of(i):
        d, away = lax.rem(i, 2), lax.div(i, 2)
        return d * RING + lax.rem(jnp.where(d == 0, places[0], places[1]) + jnp.where(away == 2, 3, jnp.where(away == 3, 2, away)), RING)

    def out_copy(i, ref, slot):
        lanes = pl.ds(pl.multiple_of(chunk_of(i) * width, width), width)
        return pltpu.make_async_copy(ref, out_hbm.at[:, lanes], sem.at[slot])

    for i in range(2):
        out_copy(i, c_ref.at[chunk_of(i)], slots + i).start()

    def step(i, carry, first):
        slot = lax.rem(i, slots)

        @pl.when(i >= slots + 2)
        def _():
            out_copy(i - slots, stage.at[slot], slot).wait()

        right = stacked_halves(res, chunk_of(i), first, depth - first)
        for p in range(pieces):
            rows = slice(p * size, (p + 1) * size)
            stage[slot, rows] = c_ref[chunk_of(i), rows] - dot(w_ref[rows, 3 * first:], right)
        out_copy(i, stage.at[slot], slot).start()
        return carry

    lax.fori_loop(2, 6, functools.partial(step, first=HALF), 0)
    lax.fori_loop(6, chunks, functools.partial(step, first=0), 0)
    for i in range(2):
        out_copy(i, c_ref.at[chunk_of(i)], slots + i).wait()
    for i in range(max(2, chunks - slots), chunks):
        out_copy(i, stage.at[i % slots], i % slots).wait()


def grid_shards(trailing, vectors, tfactor):
    height, columns = trailing.shape
    own, depth = vectors.shape
    chunks = 2 * RING
    width = columns // chunks
    blocks = height // own
    parts = len(PARTS)
    dma = pltpu.SemaphoreType.DMA
    vmem = pl.BlockSpec(memory_space=pltpu.VMEM)
    hbm = pl.BlockSpec(memory_space=pltpu.HBM)
    held, w_ref, res = pl.pallas_call(
        sum_kernel,
        out_shape=(
            pltpu.VMEM((chunks, height, width), F32),
            pltpu.VMEM((height, 3 * depth), BF16),
            pltpu.VMEM((chunks, depth, width), F32),
        ),
        in_specs=[hbm, hbm, hbm],
        out_specs=(vmem, vmem, vmem),
        scratch_shapes=[
            pltpu.VMEM((own, depth), F32),
            pltpu.VMEM((blocks, depth, own), F32),
            pltpu.VMEM((chunks, depth, width), F32),
            pltpu.VMEM((2, 2 * depth, own), BF16),
            pltpu.VMEM((2 * depth, 2 * own), BF16),
            pltpu.VMEM((RING, 2 * own, 2 * width), BF16),
            pltpu.VMEM((RING, 2 * own, 2 * width), BF16),
            pltpu.VMEM((2, 2, depth // 2, width), F32),
            pltpu.VMEM((2, 2, depth, width), F32),
            pltpu.VMEM((2, depth, width), F32),
            pltpu.VMEM((2, RING - 1, depth // RING, width), F32),
            pltpu.VMEM((2, depth // RING, width), F32),
            pltpu.VMEM((depth, depth), F32),
            dma((chunks,)), dma((2,)),
            dma, dma, dma((parts, V_PIECES)), dma((parts,)),
            dma((parts, 2, 2)), dma((parts, 2)), dma((parts, 2)), dma((parts, 2)),
            dma((parts, 2, RING)), dma((parts, 2, RING)), dma((parts,)), dma((parts,)),
        ],
        compiler_params=pltpu.CompilerParams(
            collective_id=0, has_side_effects=True, vmem_limit_bytes=42 << 20
        ),
    )(trailing, vectors, tfactor)
    slots = 4
    return pl.pallas_call(
        update_kernel,
        out_shape=jax.ShapeDtypeStruct((height, columns), F32),
        in_specs=[vmem, vmem, vmem],
        out_specs=hbm,
        scratch_shapes=[pltpu.VMEM((slots, height, width), F32), dma((slots + 2,))],
        compiler_params=pltpu.CompilerParams(vmem_limit_bytes=20 << 20),
    )(held, w_ref, res)


def plain_shards(trailing, vectors, tfactor):
    dot = functools.partial(jnp.dot, precision=lax.Precision.HIGH, preferred_element_type=F32)
    near_vectors = lax.all_gather(vectors, "col", axis=0, tiled=True)
    summed = lax.psum(dot(near_vectors.T, trailing), "row")
    return trailing - dot(near_vectors, dot(tfactor, summed))


def solution(mesh):
    placed = (P("row", "col"), P(("row", "col"), None), P())
    fits = mesh.shape["row"] == 2 * RING * RING and mesh.shape["col"] == 4

    def shards(trailing, vectors, tfactor):
        if fits and trailing.shape == (2048, 2048) and vectors.shape == (512, 256):
            return grid_shards(trailing, vectors, tfactor)
        return plain_shards(trailing, vectors, tfactor)

    return jax.shard_map(
        shards, mesh=mesh, in_specs=placed, out_specs=P("row", "col"), check_vma=False
    )
```
